256 devices in a mesh: blk: 4 (over y_lo, core), layer: 8 (over z), shard: 8 (over x, y_hi).
Axes of the slice: x: 4, y: 4 (y_hi: 2, y_lo: 2; y = y_hi * 2 + y_lo), z: 8, core: 2. Of those that a mesh axis runs over, the one named last changes fastest.
Arguments:
- train_grads: bfloat16 [32768, 8, 4096], P(('blk', 'shard'), 'layer'), may hold values from -6 to 6
- query_grads: bfloat16 [1024, 8, 4096], P(('blk', 'shard'), 'layer'), may hold values from -6 to 6
- in_factor: bfloat16 [8, 64, 64], P('layer'), as said below
- out_factor: bfloat16 [8, 64, 64], P('layer'), as said below
Outputs:
- scores: float32 [1024, 32768], P('layer', ('blk', 'shard'))
The draws below stay inside these ranges and needn't reach their ends.
Inputs may be any that keep to these rules, and one draw needn't show every extreme that they name: `in_factor`: Symmetric, with a dominant positive diagonal. `out_factor`: Symmetric, with a dominant positive diagonal.
All inputs are finite; a program needn't handle non-finite values.
Results may differ from the reference program's by a relative error of at most 0.012.
Values may be sent and summed in bfloat16 or wider, within the bound.
No kernel may reach another device: no remote copies, remote signals or barrier semaphores. Data moves between devices by JAX's collectives and lax.ppermute only.
A program may use at most 64 MiB of HBM per device.

```python
import jax
import jax.numpy as jnp
from jax import lax

PROJ = 64
GRAD = 4096
LAYERS = 8
NTRAIN = 32768
NQUERY = 1024


def factor_matrix(key, salt):
    inner = jax.random.fold_in(key, salt)
    first, second = jax.random.split(inner)
    diag = jax.random.uniform(first, (LAYERS, PROJ), jnp.float32, 1.0, 2.0)
    noise = jax.random.normal(second, (LAYERS, PROJ, PROJ), jnp.float32) * 0.06
    mirror = (noise + jnp.swapaxes(noise, 1, 2)) / jnp.sqrt(2.0)
    eye = jnp.eye(PROJ, dtype=jnp.float32)
    return (mirror * (1.0 - eye) + eye * diag[:, :, None]).astype(jnp.bfloat16)


def draw_in_factor(key, part):
    return factor_matrix(key, 11)


def draw_out_factor(key, part):
    return factor_matrix(key, 23)


def strengthened(array, rng, source, target, parts, factor):
    owner, partner = [(jnp.arange(array.shape[position]) // (array.shape[position] // parts)).reshape([-1 if axis == position else 1 for axis in range(array.ndim)]) for position in (source, target)]
    chosen = jax.random.permutation(rng, parts)[partner]
    strong = (owner == chosen) | (owner == (partner + parts // 2) % parts)
    return jnp.where(strong, factor * array, array)


def block_scale(stream_key, dims, cuts, least, largest):
    loudness, own = 1.0, jax.random.fold_in(stream_key, 6)
    for position, shards_of in cuts:
        steps = jnp.exp(jax.random.uniform(jax.random.fold_in(own, position), (shards_of,), jnp.float32, least / len(cuts), largest / len(cuts)))
        loudness = loudness * jnp.repeat(steps, dims[position] // shards_of).reshape([-1 if axis == position else 1 for axis in range(len(dims))])
    return loudness


def scatter_about(key, shape, spread, reach, pieces=(), kind=jnp.bfloat16):
    entries = jax.random.normal(key, shape, jnp.float32) * spread
    if len(pieces) > 0:
        entries = block_scale(key, shape, pieces, -0.22, 0.18) * entries
    return jnp.clip(entries, min=-reach, max=reach).astype(kind)


def heavy_noise(own_key, extent, width, most, shards, heavy, kind=jnp.bfloat16):
    array = width * jax.random.normal(own_key, extent, jnp.float32)
    if shards:
        array = array * block_scale(own_key, extent, shards, -0.22, 0.18)
    return jnp.clip(strengthened(array, jax.random.fold_in(own_key, 3), *heavy), -most, most).astype(kind)


def setup_inputs(seed: int = 0) -> dict:
    key_of = jax.random.split(jax.random.key(seed), 5)
    train_grads = scatter_about(key_of[0], (NTRAIN, LAYERS, GRAD), 1.0, 6.0, ((0, 32), (1, 8)))
    query_grads = heavy_noise(key_of[1], (NQUERY, LAYERS, GRAD), 1.0, 6.0, ((0, 32), (1, 8)), (1, 0, 8, 2.0))
    in_factor = draw_in_factor(jax.random.fold_in(key_of[4], 71), 0)
    out_factor = draw_out_factor(jax.random.fold_in(key_of[4], 71), 0)
    return {"train_grads": train_grads, "query_grads": query_grads, "in_factor": in_factor, "out_factor": out_factor}


score_scale = 1.0 / 128.0


def precondition(rows, inward, outward):
    count = rows.shape[0]
    cube = rows.reshape(count, PROJ, PROJ).astype(jnp.float32)
    half = jnp.einsum("nio,op->nip", cube, outward.astype(jnp.float32)).astype(jnp.bfloat16)
    half = lax.optimization_barrier(half)
    ready = jnp.einsum("ji,nip->njp", inward.astype(jnp.float32), half.astype(jnp.float32)).astype(jnp.bfloat16)
    return ready.reshape(count, GRAD)


def reference(train_grads, query_grads, in_factor, out_factor):
    total = jnp.zeros((NQUERY, NTRAIN), jnp.float32)
    for level in range(LAYERS):
        ready = precondition(query_grads[:, level, :], in_factor[level], out_factor[level])
        term = jnp.dot(ready, train_grads[:, level, :].T, preferred_element_type=jnp.float32) * score_scale
        term = lax.optimization_barrier(term.astype(jnp.bfloat16))
        total = total + term.astype(jnp.float32)
    return total
```

```python
import itertools

import jax
import jax.numpy as jnp
from jax import lax
from jax.experimental import pallas as pl
from jax.experimental.pallas import tpu as pltpu
from jax.sharding import Mesh, PartitionSpec as P


score_scale = 1.0 / 128.0
axes = ("ylo", "core", "layer", "x", "yhi")
sizes = {"ylo": 2, "core": 2, "layer": 8, "x": 4, "yhi": 2}
row_chunks = 2
col_chunks = 2


def pairs_of(move):
    pairs = []
    for values in itertools.product(*[range(sizes[a]) for a in axes]):
        place = dict(zip(axes, values))
        index = {"z": place["layer"], "x": place["x"], "y": place["yhi"] * 2 + place["ylo"], "core": place["core"]}
        to = move(dict(index))
        there = {"layer": to["z"], "x": to["x"], "yhi": to["y"] // 2, "ylo": to["y"] % 2, "core": to["core"]}
        number = lambda p: sum_index([p[a] for a in axes])
        pairs.append((number(place), number(there)))
    return pairs


def sum_index(values):
    total = 0
    for axis, value in zip(axes, values):
        total = total * sizes[axis] + value
    return total


def shift_z(step):
    def move(p):
        p["z"] = (p["z"] + step) % 8
        return p

    return pairs_of(move)


def shift_plane(first, step):
    def move(p):
        axis = "x" if (p["core"] == 0) == first else "y"
        p[axis] = (p[axis] + step) % 4
        return p

    return pairs_of(move)


def swap_core():
    def move(p):
        p["core"] = 1 - p["core"]
        return p

    return pairs_of(move)


def send(value, pairs):
    return lax.ppermute(value, axes, pairs)


def add(a, b):
    return (a.astype(jnp.float32) + b.astype(jnp.float32)).astype(jnp.bfloat16)


def precondition(rows, inward, outward):
    count = rows.shape[0]
    proj = inward.shape[0]
    cube = rows.reshape(count, proj, proj)
    half = jnp.einsum("nio,op->nip", cube, outward, preferred_element_type=jnp.float32).astype(
        jnp.bfloat16
    )
    ready = jnp.einsum("ji,nip->njp", inward, half, preferred_element_type=jnp.float32).astype(
        jnp.bfloat16
    )
    return ready.reshape(count, proj * proj)


def product_kernel(rows, count, offsets, *refs):
    pieces, train, out, panel = refs[:count], refs[count], refs[count + 1], refs[count + 2]

    @pl.when(pl.program_id(0) == 0)
    def _():
        start = 0
        for piece in pieces:
            panel[start : start + piece.shape[0], :] = piece[...]
            start += piece.shape[0]

    total = lax.dot_general(
        panel[...], train[...], (((1,), (1,)), ((), ())), preferred_element_type=jnp.float32
    )
    total = (total * score_scale).astype(jnp.bfloat16)
    for block in range(32):
        place = pl.multiple_of(offsets[block], rows)
        out[pl.ds(place, rows), :] = total[block * rows : (block + 1) * rows, :]


def product(offsets, pieces, train, rows, first, columns):
    tile = 256
    whole = 32 * rows
    depth = train.shape[1]
    shift = first // tile
    import functools

    return pl.pallas_call(
        functools.partial(product_kernel, rows, len(pieces)),
        grid=(columns // tile,),
        out_shape=jax.ShapeDtypeStruct((whole, columns), jnp.bfloat16),
        in_specs=[pl.BlockSpec(memory_space=pltpu.SMEM)]
        + [pl.BlockSpec(piece.shape, lambda j: (0, 0)) for piece in pieces]
        + [pl.BlockSpec((tile, depth), lambda j: (j + shift, 0))],
        out_specs=pl.BlockSpec((whole, tile), lambda j: (0, j)),
        scratch_shapes=[pltpu.VMEM((whole, depth), jnp.bfloat16)],
        compiler_params=pltpu.CompilerParams(
            dimension_semantics=("arbitrary",), vmem_limit_bytes=40 * 1024 * 1024
        ),
        cost_estimate=pl.CostEstimate(
            flops=2 * whole * columns * depth,
            bytes_accessed=2 * (whole * depth + columns * depth + whole * columns),
            transcendentals=0,
        ),
        name="product",
    )(offsets, *pieces, train)


def places(rows):
    z = lax.axis_index("layer")
    x = lax.axis_index("x")
    y = lax.axis_index("yhi") * 2 + lax.axis_index("ylo")
    core = lax.axis_index("core")
    number = jnp.arange(32, dtype=jnp.int32)
    which, second, first = number // 16, (number // 4) % 4, number % 4
    step = lambda k: jnp.where(k == 0, 0, jnp.where(k == 1, 3, jnp.where(k == 2, 1, 2)))
    owner = jnp.where(which == 0, core, 1 - core)
    along_x = jnp.where(owner == 0, step(first), step(second))
    along_y = jnp.where(owner == 0, step(second), step(first))
    from_x = (x + along_x) % 4
    from_y = (y + along_y) % 4
    dest = (from_y % 2) * 4 + owner * 2 + from_x // 2
    slot = (from_x % 2) * 2 + from_y // 2
    return ((dest - z) % 8) * (4 * rows) + slot * rows


def gather_chunk(own, chunk):
    near_up = send(own, shift_plane(True, 1))
    near_down = send(own, shift_plane(True, -1))
    if chunk % 2 == 0:
        far = send(near_up, shift_plane(True, 1))
    else:
        far = send(near_down, shift_plane(True, -1))
    bundle = jnp.concatenate([own, near_up, near_down, far], axis=0)
    up = send(bundle, shift_plane(False, 1))
    down = send(bundle, shift_plane(False, -1))
    half = bundle.shape[0] // 2
    far_a = send(up[:half], shift_plane(False, 1))
    far_b = send(down[half:], shift_plane(False, -1))
    mine = [bundle, up, down, far_a, far_b]
    return mine + [send(piece, swap_core()) for piece in mine]


def reduce_chunk(partial):
    half = partial.shape[1] // 2
    below = send(partial[4, :half], shift_z(-1))
    above = send(partial[4, half:], shift_z(1))
    below = send(jnp.concatenate([add(partial[5, :half], below), partial[5, half:]]), shift_z(-1))
    above = send(jnp.concatenate([partial[3, :half], add(partial[3, half:], above)]), shift_z(1))
    below = send(add(partial[6], below), shift_z(-1))
    above = send(add(partial[2], above), shift_z(1))
    below = send(add(partial[7], below), shift_z(-1))
    above = send(add(partial[1], above), shift_z(1))
    return partial[0].astype(jnp.float32) + below.astype(jnp.float32) + above.astype(jnp.float32)


def per_device(train_grads, query_grads, in_factor, out_factor):
    train = train_grads[:, 0, :]
    ready = precondition(query_grads[:, 0, :], in_factor[0], out_factor[0])
    rows = ready.shape[0] // row_chunks
    columns = train.shape[0] // col_chunks
    offsets = places(rows)
    out = []
    for chunk in range(row_chunks):
        pieces = gather_chunk(ready[chunk * rows : (chunk + 1) * rows], chunk)
        wide = []
        for part in range(col_chunks):
            partial = product(offsets, pieces, train, rows, part * columns, columns)
            wide.append(reduce_chunk(partial.reshape(8, 4 * rows, columns)))
        out.append(jnp.concatenate(wide, axis=1).reshape(4, rows, train.shape[0]))
    return jnp.stack(out, axis=1).reshape(128, train.shape[0])


def solution(mesh):
    fine = Mesh(mesh.devices.reshape(2, 2, 8, 4, 2), axes)
    spread = ("ylo", "core", "x", "yhi")
    return jax.shard_map(
        per_device,
        mesh=fine,
        in_specs=(
            P(spread, "layer", None),
            P(spread, "layer", None),
            P("layer", None, None),
            P("layer", None, None),
        ),
        out_specs=P("layer", spread),
        check_vma=False,
    )
```

```python
import functools
import itertools

import jax
import jax.numpy as jnp
from jax import lax
from jax.experimental import pallas as pl
from jax.experimental.pallas import tpu as pltpu
from jax.sharding import Mesh, PartitionSpec as P


score_scale = 1.0 / 128.0
axes = ("ylo", "core", "layer", "x", "yhi")
sizes = {"ylo": 2, "core": 2, "layer": 8, "x": 4, "yhi": 2}
col_chunks = 2
tile = 256


def pairs_of(move):
    pairs = []
    for values in itertools.product(*[range(sizes[a]) for a in axes]):
        place = dict(zip(axes, values))
        index = {"z": place["layer"], "x": place["x"], "y": place["yhi"] * 2 + place["ylo"], "core": place["core"]}
        to = move(dict(index))
        there = {"layer": to["z"], "x": to["x"], "yhi": to["y"] // 2, "ylo": to["y"] % 2, "core": to["core"]}
        number = lambda p: sum_index([p[a] for a in axes])
        pairs.append((number(place), number(there)))
    return pairs


def sum_index(values):
    total = 0
    for axis, value in zip(axes, values):
        total = total * sizes[axis] + value
    return total


def chain():
    def move(p):
        p["z"] = (p["z"] + (1 if p["core"] else -1)) % 8
        return p

    return pairs_of(move)


def shift_plane(first, step):
    def move(p):
        axis = "x" if (p["core"] == 0) == first else "y"
        p[axis] = (p[axis] + step) % 4
        return p

    return pairs_of(move)


def swap_core():
    def move(p):
        p["core"] = 1 - p["core"]
        return p

    return pairs_of(move)


def send(value, pairs):
    return lax.ppermute(value, axes, pairs)


def add(a, b):
    return (a.astype(jnp.float32) + b.astype(jnp.float32)).astype(jnp.bfloat16)


def precondition(rows, inward, outward):
    count = rows.shape[0]
    proj = inward.shape[0]
    cube = rows.reshape(count, proj, proj)
    half = jnp.einsum("nio,op->nip", cube, outward, preferred_element_type=jnp.float32).astype(
        jnp.bfloat16
    )
    ready = jnp.einsum("ji,nip->njp", inward, half, preferred_element_type=jnp.float32).astype(
        jnp.bfloat16
    )
    return ready.reshape(count, proj * proj)


def flip_kernel(train, out, tiles, sems):
    copies = [
        pltpu.make_async_copy(train.at[pl.ds(j * tile, tile), :], tiles.at[j], sems.at[j])
        for j in range(train.shape[0] // tile)
    ]
    for copy in copies:
        copy.start()
    for j, copy in enumerate(copies):
        copy.wait()
        out[:, j * tile : (j + 1) * tile] = tiles[j].T


def flip(train):
    count, depth = train.shape
    return pl.pallas_call(
        flip_kernel,
        out_shape=jax.ShapeDtypeStruct((depth, count), jnp.bfloat16),
        in_specs=[pl.BlockSpec(memory_space=pltpu.HBM)],
        out_specs=pl.BlockSpec(memory_space=pltpu.VMEM),
        scratch_shapes=[
            pltpu.VMEM((count // tile, tile, depth), jnp.bfloat16),
            pltpu.SemaphoreType.DMA((count // tile,)),
        ],
        compiler_params=pltpu.CompilerParams(vmem_limit_bytes=24 * 1024 * 1024),
        cost_estimate=pl.CostEstimate(flops=4000000000, bytes_accessed=4 * count * depth, transcendentals=0),
        name="flip",
    )(pltpu.with_memory_space_constraint(train, pltpu.HBM))


def multiply(pieces, train, panel, first, columns, store):
    start = 0
    for piece in pieces:
        panel[start : start + piece.shape[0], :] = piece[...]
        start += piece.shape[0]

    def one(j, carry):
        lanes = pl.ds(pl.multiple_of(first + j * tile, tile), tile)
        total = jnp.dot(panel[...], train[:, lanes], preferred_element_type=jnp.float32)
        store(pl.ds(pl.multiple_of(j * tile, tile), tile), (total * score_scale).astype(jnp.bfloat16))
        return carry

    lax.fori_loop(0, columns // tile, one, 0)


def early_kernel(count, *refs):
    pieces, (train, out, panel) = refs[:count], refs[count:]

    def store(lanes, total):
        out[:, lanes] = total

    multiply(pieces, train, panel, 0, out.shape[1], store)


def late_kernel(count, early, rows, first, offsets, *refs):
    pieces, ready, (train, out, panel) = refs[:count], refs[count : count + early], refs[count + early :]
    columns = out.shape[1]

    def place(block):
        return pl.ds(pl.multiple_of(offsets[block], rows), rows)

    block = 0
    for source in ready:
        for start in range(0, source.shape[0], rows):
            out[place(block), :] = source[start : start + rows, first : first + columns]
            block += 1

    def store(lanes, total):
        for number in range(total.shape[0] // rows):
            out[place(block + number), lanes] = total[number * rows : (number + 1) * rows, :]

    multiply(pieces, train, panel, first, columns, store)


def call(kernel, name, scalars, inputs, train, whole, height, columns):
    depth = train.shape[0]
    return pl.pallas_call(
        kernel,
        out_shape=jax.ShapeDtypeStruct((height, columns), jnp.bfloat16),
        in_specs=[pl.BlockSpec(memory_space=pltpu.SMEM) for _ in scalars]
        + [pl.BlockSpec(memory_space=pltpu.VMEM) for _ in inputs]
        + [pl.BlockSpec(memory_space=pltpu.VMEM)],
        out_specs=pl.BlockSpec(memory_space=pltpu.VMEM),
        scratch_shapes=[pltpu.VMEM((whole, depth), jnp.bfloat16)],
        compiler_params=pltpu.CompilerParams(vmem_limit_bytes=10 * 1024 * 1024),
        cost_estimate=pl.CostEstimate(
            flops=2 * whole * columns * depth,
            bytes_accessed=2 * (whole * depth + columns * depth + whole * columns),
            transcendentals=0,
        ),
        name=name,
    )(*scalars, *inputs, train)


def early_product(pieces, train):
    whole = sum(piece.shape[0] for piece in pieces)
    kernel = functools.partial(early_kernel, len(pieces))
    return call(kernel, "early_product", [], pieces, train, whole, whole, train.shape[1])


def late_product(offsets, pieces, ready, train, rows, first, columns):
    whole = sum(piece.shape[0] for piece in pieces)
    kernel = functools.partial(late_kernel, len(pieces), len(ready), rows, first)
    height = whole + sum(piece.shape[0] for piece in ready)
    return call(kernel, "late_product", [offsets], [*pieces, *ready], train, whole, height, columns)


first_steps = (0, 1, -1, 2)
order = (
    [(0, f, 0) for f in first_steps]
    + [(1, f, 0) for f in first_steps]
    + [(0, f, 1) for f in first_steps]
    + [(1, f, 1) for f in first_steps]
    + [(0, f, -1) for f in first_steps]
    + [(1, f, -1) for f in first_steps]
    + [(0, f, 2) for f in first_steps]
    + [(1, f, 2) for f in first_steps]
)


def places(rows):
    z = lax.axis_index("layer")
    x = lax.axis_index("x")
    y = lax.axis_index("yhi") * 2 + lax.axis_index("ylo")
    core = lax.axis_index("core")
    other = jnp.asarray([o[0] for o in order], jnp.int32)
    first = jnp.asarray([o[1] for o in order], jnp.int32)
    second = jnp.asarray([o[2] for o in order], jnp.int32)
    owner = jnp.where(other == 0, core, 1 - core)
    from_x = (x + 4 - jnp.where(owner == 0, first, second)) % 4
    from_y = (y + 4 - jnp.where(owner == 0, second, first)) % 4
    dest = (from_y % 2) * 4 + owner * 2 + from_x // 2
    slot = (from_x % 2) * 2 + from_y // 2
    ahead = jnp.where(core == 0, dest - z + 8, z - dest + 8) % 8
    group = jnp.where(ahead >= 4, ahead - 4, 7 - ahead)
    return group * (4 * rows) + slot * rows


def tie(values, *others):
    tied = lax.optimization_barrier((tuple(values), others))
    return list(tied[0])


def first_round(partial):
    given = send(partial[4:7], swap_core())
    moving = send(partial[0], chain())
    return jnp.stack([add(partial[1], moving), given[0]]), given


def next_round(partial, given, moving, step):
    moving = send(moving, chain())
    return jnp.stack([add(partial[step], moving[0]), add(given[step - 1], moving[1])])


def last_round(partial, moving):
    moving = send(moving, chain())
    back = send(moving[1], swap_core())
    return partial[7].astype(jnp.float32) + moving[0].astype(jnp.float32) + back.astype(jnp.float32)


def per_device(train_grads, query_grads, in_factor, out_factor):
    own = precondition(query_grads[:, 0, :], in_factor[0], out_factor[0])
    rows = own.shape[0]
    offsets, own = tie([places(rows), own])
    near = [own] + [send(own, shift_plane(True, step)) for step in (1, -1, 2)]
    train = flip(train_grads[:, 0, :])
    bundle = jnp.concatenate(tie(near, train), axis=0)
    up = send(bundle, shift_plane(False, 1))
    down = send(bundle, shift_plane(False, -1))
    half = 2 * rows
    first = early_product([bundle, send(bundle, swap_core())], train)
    up, down = tie([up, down], first)
    far = [send(up[:half], shift_plane(False, 1)), send(down[half:], shift_plane(False, -1))]
    second = early_product([up, send(up, swap_core()), down, send(down, swap_core())], train)
    far = tie(far, second)
    far = far + [send(piece, swap_core()) for piece in far]
    partials = []
    columns = train.shape[1] // col_chunks
    for part in range(col_chunks):
        if part:
            far = tie(far, partials[0])
        partials.append(
            late_product(offsets, far, [first, second], train, rows, part * columns, columns)
        )
    blocks = [p.reshape(8, 4 * rows, p.shape[1]) for p in partials]
    rounds = [first_round(b) for b in blocks]
    moving = [r[0] for r in rounds]
    for step in (2, 3):
        moving = [next_round(b, r[1], m, step) for b, r, m in zip(blocks, rounds, moving)]
    return jnp.concatenate([last_round(b, m) for b, m in zip(blocks, moving)], axis=1)


def solution(mesh):
    fine = Mesh(mesh.devices.reshape(2, 2, 8, 4, 2), axes)
    spread = ("ylo", "core", "x", "yhi")
    return jax.shard_map(
        per_device,
        mesh=fine,
        in_specs=(
            P(spread, "layer", None),
            P(spread, "layer", None),
            P("layer", None, None),
            P("layer", None, None),
        ),
        out_specs=P("layer", spread),
        check_vma=False,
    )
```

```python
import functools
import itertools

import jax
import jax.numpy as jnp
from jax import lax
from jax.experimental import pallas as pl
from jax.experimental.pallas import tpu as pltpu
from jax.sharding import Mesh, PartitionSpec as P


score_scale = 1.0 / 128.0
axes = ("ylo", "core", "layer", "x", "yhi")
sizes = {"ylo": 2, "core": 2, "layer": 8, "x": 4, "yhi": 2}
col_chunks = 2
tile = 256


def pairs_of(move):
    pairs = []
    for values in itertools.product(*[range(sizes[a]) for a in axes]):
        place = dict(zip(axes, values))
        index = {"z": place["layer"], "x": place["x"], "y": place["yhi"] * 2 + place["ylo"], "core": place["core"]}
        to = move(dict(index))
        there = {"layer": to["z"], "x": to["x"], "yhi": to["y"] // 2, "ylo": to["y"] % 2, "core": to["core"]}
        number = lambda p: sum_index([p[a] for a in axes])
        pairs.append((number(place), number(there)))
    return pairs


def sum_index(values):
    total = 0
    for axis, value in zip(axes, values):
        total = total * sizes[axis] + value
    return total


def chain():
    def move(p):
        p["z"] = (p["z"] + (1 if p["core"] else -1)) % 8
        return p

    return pairs_of(move)


def shift_plane(first, step):
    def move(p):
        axis = "x" if (p["core"] == 0) == first else "y"
        p[axis] = (p[axis] + step) % 4
        return p

    return pairs_of(move)


def swap_core():
    def move(p):
        p["core"] = 1 - p["core"]
        return p

    return pairs_of(move)


def send(value, pairs):
    return lax.ppermute(value, axes, pairs)


def add(a, b):
    return (a.astype(jnp.float32) + b.astype(jnp.float32)).astype(jnp.bfloat16)


def precondition(rows, inward, outward):
    count = rows.shape[0]
    proj = inward.shape[0]
    cube = rows.reshape(count, proj, proj)
    half = jnp.einsum("nio,op->nip", cube, outward, preferred_element_type=jnp.float32).astype(
        jnp.bfloat16
    )
    ready = jnp.einsum("ji,nip->njp", inward, half, preferred_element_type=jnp.float32).astype(
        jnp.bfloat16
    )
    return ready.reshape(count, proj * proj)


def flip_kernel(train, out, tiles, sems):
    copies = [
        pltpu.make_async_copy(train.at[pl.ds(j * tile, tile), :], tiles.at[j], sems.at[j])
        for j in range(train.shape[0] // tile)
    ]
    for copy in copies:
        copy.start()
    for j, copy in enumerate(copies):
        copy.wait()
        out[:, j * tile : (j + 1) * tile] = tiles[j].T


def flip(train):
    count, depth = train.shape
    return pl.pallas_call(
        flip_kernel,
        out_shape=jax.ShapeDtypeStruct((depth, count), jnp.bfloat16),
        in_specs=[pl.BlockSpec(memory_space=pltpu.HBM)],
        out_specs=pl.BlockSpec(memory_space=pltpu.VMEM),
        scratch_shapes=[
            pltpu.VMEM((count // tile, tile, depth), jnp.bfloat16),
            pltpu.SemaphoreType.DMA((count // tile,)),
        ],
        compiler_params=pltpu.CompilerParams(vmem_limit_bytes=24 * 1024 * 1024),
        cost_estimate=pl.CostEstimate(flops=4000000000, bytes_accessed=4 * count * depth, transcendentals=0),
        name="flip",
    )(pltpu.with_memory_space_constraint(train, pltpu.HBM))


def multiply(pieces, train, panel, first, columns, store):
    start = 0
    for piece in pieces:
        panel[start : start + piece.shape[0], :] = piece[...]
        start += piece.shape[0]

    def one(j, carry):
        lanes = pl.ds(pl.multiple_of(first + j * tile, tile), tile)
        total = jnp.dot(panel[...], train[:, lanes], preferred_element_type=jnp.float32)
        store(pl.ds(pl.multiple_of(j * tile, tile), tile), (total * score_scale).astype(jnp.bfloat16))
        return carry

    lax.fori_loop(0, columns // tile, one, 0)


def early_kernel(count, *refs):
    pieces, (train, out, panel) = refs[:count], refs[count:]

    def store(lanes, total):
        out[:, lanes] = total

    multiply(pieces, train, panel, 0, out.shape[1], store)


def late_kernel(count, early, rows, first, offsets, *refs):
    pieces, ready, (train, out, panel) = refs[:count], refs[count : count + early], refs[count + early :]
    columns = out.shape[1]

    def place(block):
        return pl.ds(pl.multiple_of(offsets[block], rows), rows)

    block = 0
    for source in ready:
        for start in range(0, source.shape[0], rows):
            out[place(block), :] = source[start : start + rows, first : first + columns]
            block += 1

    def store(lanes, total):
        for number in range(total.shape[0] // rows):
            out[place(block + number), lanes] = total[number * rows : (number + 1) * rows, :]

    multiply(pieces, train, panel, first, columns, store)


def call(kernel, scalars, inputs, train, whole, height, columns):
    depth = train.shape[0]
    return pl.pallas_call(
        kernel,
        out_shape=jax.ShapeDtypeStruct((height, columns), jnp.bfloat16),
        in_specs=[pl.BlockSpec(memory_space=pltpu.SMEM) for _ in scalars]
        + [pl.BlockSpec(memory_space=pltpu.VMEM) for _ in inputs]
        + [pl.BlockSpec(memory_space=pltpu.VMEM)],
        out_specs=pl.BlockSpec(memory_space=pltpu.VMEM),
        scratch_shapes=[pltpu.VMEM((whole, depth), jnp.bfloat16)],
        compiler_params=pltpu.CompilerParams(vmem_limit_bytes=10 * 1024 * 1024),
        cost_estimate=pl.CostEstimate(
            flops=2 * whole * columns * depth,
            bytes_accessed=2 * (whole * depth + columns * depth + whole * columns),
            transcendentals=0,
        ),
    )(*scalars, *inputs, train)


def early_product(pieces, train):
    whole = sum(piece.shape[0] for piece in pieces)
    kernel = functools.partial(early_kernel, len(pieces))
    return call(kernel, [], pieces, train, whole, whole, train.shape[1])


def late_product(offsets, pieces, ready, train, rows, first, columns):
    whole = sum(piece.shape[0] for piece in pieces)
    kernel = functools.partial(late_kernel, len(pieces), len(ready), rows, first)
    height = whole + sum(piece.shape[0] for piece in ready)
    return call(kernel, [offsets], [*pieces, *ready], train, whole, height, columns)


steps_x, steps_y = (0, 1), (-1, 2)
order = [
    (other, first, second)
    for other, firsts, second in (
        (0, steps_x, 0),
        (0, steps_y, 0),
        (1, steps_x, 0),
        (1, steps_y, 0),
        (0, steps_x, 1),
        (1, steps_x, 1),
        (0, steps_x, -1),
        (1, steps_x, -1),
        (0, steps_y, 1),
        (1, steps_y, 1),
        (0, steps_y, -1),
        (1, steps_y, -1),
        (0, steps_x, 2),
        (1, steps_x, 2),
        (0, steps_y, 2),
        (1, steps_y, 2),
    )
    for first in firsts
]


def places_of_device():
    y = lax.axis_index("yhi") * 2 + lax.axis_index("ylo")
    return lax.axis_index("layer"), lax.axis_index("x"), y, lax.axis_index("core")


def places(rows, z, x, y, core):
    other = jnp.asarray([o[0] for o in order], jnp.int32)
    first = jnp.asarray([o[1] for o in order], jnp.int32)
    second = jnp.asarray([o[2] for o in order], jnp.int32)
    owner = jnp.where(other == 0, core, 1 - core)
    from_x = (x + 4 - jnp.where(owner == 0, first, second)) % 4
    from_y = (y + 4 - jnp.where(owner == 0, second, first)) % 4
    dest = (from_y % 2) * 4 + owner * 2 + from_x // 2
    slot = (from_x % 2) * 2 + from_y // 2
    ahead = jnp.where(core == 0, dest - z + 8, z - dest + 8) % 8
    group = jnp.where(ahead >= 4, ahead - 4, 7 - ahead)
    return group * (4 * rows) + slot * rows


def tie(values, *others):
    tied = lax.optimization_barrier((tuple(values), others))
    return list(tied[0])


def first_round(partial):
    given = send(partial[4:7], swap_core())
    moving = send(partial[0], chain())
    return jnp.stack([add(partial[1], moving), given[0]]), given


def next_round(partial, given, moving, step):
    moving = send(moving, chain())
    return jnp.stack([add(partial[step], moving[0]), add(given[step - 1], moving[1])])


def last_round(partial, moving):
    moving = send(moving, chain())
    back = send(moving[1], swap_core())
    return partial[7].astype(jnp.float32) + moving[0].astype(jnp.float32) + back.astype(jnp.float32)


def scored(train_grads, query_grads, in_factor, out_factor):
    position, queries = tie([places_of_device(), query_grads[:, 0, :]])
    own = precondition(queries, in_factor[0], out_factor[0])
    rows = own.shape[0]
    near = send(own, shift_plane(True, 1))
    back = send(own, shift_plane(True, -1))
    far = send(own, shift_plane(True, 2))
    offsets = places(rows, *position)
    train = flip(train_grads[:, 0, :])
    here_x = jnp.concatenate([own, near], axis=0)
    here_y = jnp.concatenate([back, far], axis=0)
    up_x = send(here_x, shift_plane(False, 1))
    down_x = send(here_x, shift_plane(False, -1))
    up_y = send(here_y, shift_plane(False, 1))
    down_y = send(here_y, shift_plane(False, -1))
    swap = lambda value: send(value, swap_core())
    far_x = send(up_x, shift_plane(False, 1))
    far_y = send(down_y, shift_plane(False, -1))
    ready = []

    def early(pieces):
        ready.append(early_product(pieces, train))

    early([here_x, here_y])
    early([swap(here_x), swap(here_y), up_x, swap(up_x), down_x, swap(down_x)])
    early([up_y, swap(up_y), down_y, swap(down_y)])
    early([far_x, swap(far_x)])
    last = [far_y, swap(far_y)]
    partials = []
    columns = train.shape[1] // col_chunks
    for part in range(col_chunks):
        if part:
            last = tie(last, partials[0])
        partials.append(
            late_product(offsets, last, ready, train, rows, part * columns, columns)
        )
    blocks = [p.reshape(8, 4 * rows, p.shape[1]) for p in partials]
    rounds = [first_round(b) for b in blocks]
    moving = [r[0] for r in rounds]
    for step in (2, 3):
        moving = [next_round(b, r[1], m, step) for b, r, m in zip(blocks, rounds, moving)]
    return jnp.concatenate([last_round(b, m) for b, m in zip(blocks, moving)], axis=1)


def solution(mesh):
    fine = Mesh(mesh.devices.reshape(2, 2, 8, 4, 2), axes)
    spread = ("ylo", "core", "x", "yhi")
    return jax.shard_map(
        scored,
        mesh=fine,
        in_specs=(
            P(spread, "layer", None),
            P(spread, "layer", None),
            P("layer", None, None),
            P("layer", None, None),
        ),
        out_specs=P("layer", spread),
        check_vma=False,
    )
```

```python
import functools
import itertools

import jax
import jax.numpy as jnp
from jax import lax
from jax.experimental import pallas as pl
from jax.experimental.pallas import tpu as pltpu
from jax.sharding import Mesh, PartitionSpec as P


score_scale = 1.0 / 128.0
axes = ("ylo", "core", "layer", "x", "yhi")
sizes = {"ylo": 2, "core": 2, "layer": 8, "x": 4, "yhi": 2}
widths = (512, 512)
tile = 256


def pairs_of(move):
    pairs = []
    for values in itertools.product(*[range(sizes[a]) for a in axes]):
        place = dict(zip(axes, values))
        index = {"z": place["layer"], "x": place["x"], "y": place["yhi"] * 2 + place["ylo"], "core": place["core"]}
        to = move(dict(index))
        there = {"layer": to["z"], "x": to["x"], "yhi": to["y"] // 2, "ylo": to["y"] % 2, "core": to["core"]}
        number = lambda p: sum_index([p[a] for a in axes])
        pairs.append((number(place), number(there)))
    return pairs


def sum_index(values):
    total = 0
    for axis, value in zip(axes, values):
        total = total * sizes[axis] + value
    return total


def chain():
    def move(p):
        p["z"] = (p["z"] + (1 if p["core"] else -1)) % 8
        return p

    return pairs_of(move)


def shift_plane(first, step):
    def move(p):
        axis = "x" if (p["core"] == 0) == first else "y"
        p[axis] = (p[axis] + step) % 4
        return p

    return pairs_of(move)


def swap_core():
    def move(p):
        p["core"] = 1 - p["core"]
        return p

    return pairs_of(move)


def send(value, pairs):
    return lax.ppermute(value, axes, pairs)


def add(a, b):
    return (a.astype(jnp.float32) + b.astype(jnp.float32)).astype(jnp.bfloat16)


def precondition(rows, inward, outward):
    count = rows.shape[0]
    proj = inward.shape[0]
    cube = rows.reshape(count, proj, proj)
    half = jnp.einsum("nio,op->nip", cube, outward, preferred_element_type=jnp.float32).astype(
        jnp.bfloat16
    )
    ready = jnp.einsum("ji,nip->njp", inward, half, preferred_element_type=jnp.float32).astype(
        jnp.bfloat16
    )
    return ready.reshape(count, proj * proj)


def flip_kernel(train, out, tiles, sems):
    copies = [
        pltpu.make_async_copy(train.at[pl.ds(j * tile, tile), :], tiles.at[j], sems.at[j])
        for j in range(train.shape[0] // tile)
    ]
    for copy in copies:
        copy.start()
    for j, copy in enumerate(copies):
        copy.wait()
        out[:, j * tile : (j + 1) * tile] = tiles[j].T


def flip(train):
    count, depth = train.shape
    return pl.pallas_call(
        flip_kernel,
        out_shape=jax.ShapeDtypeStruct((depth, count), jnp.bfloat16),
        in_specs=[pl.BlockSpec(memory_space=pltpu.HBM)],
        out_specs=pl.BlockSpec(memory_space=pltpu.VMEM),
        scratch_shapes=[
            pltpu.VMEM((count // tile, tile, depth), jnp.bfloat16),
            pltpu.SemaphoreType.DMA((count // tile,)),
        ],
        compiler_params=pltpu.CompilerParams(vmem_limit_bytes=24 * 1024 * 1024),
        cost_estimate=pl.CostEstimate(flops=4000000000, bytes_accessed=4 * count * depth, transcendentals=0),
        name="flip",
    )(pltpu.with_memory_space_constraint(train, pltpu.HBM))


def multiply(pieces, train, panel, first, columns, store):
    start = 0
    for piece in pieces:
        panel[start : start + piece.shape[0], :] = piece[...]
        start += piece.shape[0]

    size = tile if columns % tile == 0 else columns

    def one(j, carry):
        lanes = pl.ds(pl.multiple_of(first + j * size, 128), size)
        total = jnp.dot(panel[...], train[:, lanes], preferred_element_type=jnp.float32)
        store(pl.ds(pl.multiple_of(j * size, 128), size), (total * score_scale).astype(jnp.bfloat16))
        return carry

    lax.fori_loop(0, columns // size, one, 0)


def early_kernel(count, *refs):
    pieces, (train, out, panel) = refs[:count], refs[count:]

    def store(lanes, total):
        out[:, lanes] = total

    multiply(pieces, train, panel, 0, out.shape[1], store)


def late_kernel(count, early, rows, first, offsets, *refs):
    pieces, ready, (train, out, panel) = refs[:count], refs[count : count + early], refs[count + early :]
    columns = out.shape[1]

    def place(block):
        return pl.ds(pl.multiple_of(offsets[block], rows), rows)

    block = 0
    for source in ready:
        for start in range(0, source.shape[0], rows):
            out[place(block), :] = source[start : start + rows, first : first + columns]
            block += 1

    def store(lanes, total):
        for number in range(total.shape[0] // rows):
            out[place(block + number), lanes] = total[number * rows : (number + 1) * rows, :]

    multiply(pieces, train, panel, first, columns, store)


def call(kernel, scalars, inputs, train, whole, height, columns):
    depth = train.shape[0]
    return pl.pallas_call(
        kernel,
        out_shape=jax.ShapeDtypeStruct((height, columns), jnp.bfloat16),
        in_specs=[pl.BlockSpec(memory_space=pltpu.SMEM) for _ in scalars]
        + [pl.BlockSpec(memory_space=pltpu.VMEM) for _ in inputs]
        + [pl.BlockSpec(memory_space=pltpu.VMEM)],
        out_specs=pl.BlockSpec(memory_space=pltpu.VMEM),
        scratch_shapes=[pltpu.VMEM((whole, depth), jnp.bfloat16)],
        compiler_params=pltpu.CompilerParams(vmem_limit_bytes=10 * 1024 * 1024),
        cost_estimate=pl.CostEstimate(
            flops=2 * whole * columns * depth,
            bytes_accessed=2 * (whole * depth + columns * depth + whole * columns),
            transcendentals=0,
        ),
    )(*scalars, *inputs, train)


def early_product(pieces, train):
    whole = sum(piece.shape[0] for piece in pieces)
    kernel = functools.partial(early_kernel, len(pieces))
    return call(kernel, [], pieces, train, whole, whole, train.shape[1])


def late_product(offsets, pieces, ready, train, rows, first, columns):
    whole = sum(piece.shape[0] for piece in pieces)
    kernel = functools.partial(late_kernel, len(pieces), len(ready), rows, first)
    height = whole + sum(piece.shape[0] for piece in ready)
    return call(kernel, [offsets], [*pieces, *ready], train, whole, height, columns)


steps_x, steps_y = (0, 1), (-1, 2)
order = [
    (other, first, second)
    for other, firsts, second in (
        (0, steps_x, 0),
        (0, steps_y, 0),
        (1, steps_x, 0),
        (1, steps_y, 0),
        (0, steps_x, 1),
        (1, steps_x, 1),
        (0, steps_x, -1),
        (1, steps_x, -1),
        (0, steps_y, 1),
        (1, steps_y, 1),
        (0, steps_y, -1),
        (1, steps_y, -1),
        (0, steps_x, 2),
        (1, steps_x, 2),
        (0, steps_y, 2),
        (1, steps_y, 2),
    )
    for first in firsts
]


def places_of_device():
    y = lax.axis_index("yhi") * 2 + lax.axis_index("ylo")
    return lax.axis_index("layer"), lax.axis_index("x"), y, lax.axis_index("core")


def places(rows, z, x, y, core):
    other = jnp.asarray([o[0] for o in order], jnp.int32)
    first = jnp.asarray([o[1] for o in order], jnp.int32)
    second = jnp.asarray([o[2] for o in order], jnp.int32)
    owner = jnp.where(other == 0, core, 1 - core)
    from_x = (x + 4 - jnp.where(owner == 0, first, second)) % 4
    from_y = (y + 4 - jnp.where(owner == 0, second, first)) % 4
    dest = (from_y % 2) * 4 + owner * 2 + from_x // 2
    slot = (from_x % 2) * 2 + from_y // 2
    ahead = jnp.where(core == 0, dest - z + 8, z - dest + 8) % 8
    group = jnp.where(ahead >= 4, ahead - 4, 7 - ahead)
    return group * (4 * rows) + slot * rows


def tie(values, *others):
    tied = lax.optimization_barrier((tuple(values), others))
    return list(tied[0])


def first_round(partial):
    moving = send(partial[0], chain())
    given = send(partial[4:7], swap_core())
    return jnp.stack([add(partial[1], moving), given[0]]), given


def next_round(partial, given, moving, step):
    moving = send(moving, chain())
    return jnp.stack([add(partial[step], moving[0]), add(given[step - 1], moving[1])])


def last_round(partial, moving):
    moving = send(moving, chain())
    back = send(moving[1], swap_core())
    return partial[7].astype(jnp.float32) + moving[0].astype(jnp.float32) + back.astype(jnp.float32)


def scored(train_grads, query_grads, in_factor, out_factor):
    position, queries = tie([places_of_device(), query_grads[:, 0, :]])
    own = precondition(queries, in_factor[0], out_factor[0])
    rows = own.shape[0]
    near = send(own, shift_plane(True, 1))
    back = send(own, shift_plane(True, -1))
    far = send(own, shift_plane(True, 2))
    offsets = places(rows, *position)
    train = flip(train_grads[:, 0, :])
    here_x = jnp.concatenate([own, near], axis=0)
    here_y = jnp.concatenate([back, far], axis=0)
    up_x = send(here_x, shift_plane(False, 1))
    down_x = send(here_x, shift_plane(False, -1))
    up_y = send(here_y, shift_plane(False, 1))
    down_y = send(here_y, shift_plane(False, -1))
    swap = lambda value: send(value, swap_core())
    far_x = send(up_x, shift_plane(False, 1))
    far_y = send(down_y, shift_plane(False, -1))
    ready = []

    def early(pieces):
        ready.append(early_product(pieces, train))

    early([here_x, here_y, swap(here_x), swap(here_y), up_x, swap(up_x), down_x, swap(down_x)])
    early([up_y, swap(up_y), down_y, swap(down_y)])
    early([far_x, swap(far_x)])
    last = [far_y, swap(far_y)]
    partials = []
    for part, columns in enumerate(widths):
        if part:
            last = tie(last, partials[-1])
        partials.append(
            late_product(offsets, last, ready, train, rows, sum(widths[:part]), columns)
        )
    blocks = [p.reshape(8, 4 * rows, p.shape[1]) for p in partials]
    rounds = [first_round(b) for b in blocks]
    moving = [r[0] for r in rounds]
    for step in (2, 3):
        moving = [
            next_round(b, r[1], m, step)
            for b, r, m in zip(blocks, rounds, moving)
        ]
    return jnp.concatenate([last_round(b, m) for b, m in zip(blocks, moving)], axis=1)


def solution(mesh):
    fine = Mesh(mesh.devices.reshape(2, 2, 8, 4, 2), axes)
    spread = ("ylo", "core", "x", "yhi")
    return jax.shard_map(
        scored,
        mesh=fine,
        in_specs=(
            P(spread, "layer", None),
            P(spread, "layer", None),
            P("layer", None, None),
            P("layer", None, None),
        ),
        out_specs=P("layer", spread),
        check_vma=False,
    )
```
